32 devices in a mesh: row: 4 (over z), col: 8 (over y, x, core).
Axes of the slice: x: 2, y: 2, z: 4, core: 2. Of those that a mesh axis runs over, the one named last changes fastest.
Arguments:
- a_matrix: bfloat16 [8192, 8192], P('row', 'col'), may hold values from -6 to 6
- a_flags: int32 [64, 64], P('row', 'col'), may hold values from 0 to 1, as said below
- b_matrix: bfloat16 [8192, 16384], P('row', 'col'), may hold values from -0.1875 to 0.1875
- b_flags: int32 [64, 128], P('row', 'col'), may hold values from 0 to 1, as said below
- sections: int32 [2], replicated, may hold values from 0 to 7
Outputs:
- packed: bfloat16 [8192, 16384], P('row', 'col')
- tile_place: int32 [64, 128], P('row', 'col')
The draws below stay inside these ranges and needn't reach their ends.
Inputs may be any that keep to these rules, and one draw needn't show every extreme that they name: `a_flags`: 0 or 1; the 16 x 8 tiles of one device hold at most 64 ones, and some device holds exactly 64. `b_flags`: 0 or 1; each aligned block of 8 x 16 tiles holds at most 64 ones, and some block exactly 64.
All inputs are finite; a program needn't handle non-finite values.
Results may differ from the reference program's by a relative error of at most 0.001.
Values may be sent and summed in bfloat16 or wider, within the bound.
A program may use at most 128 MiB of HBM per device.

```python
import jax
import jax.numpy as jnp
from jax import lax

TILE = 128
TM_DEV = 16
TN_DEV = 16
KT = 8
SECTIONS = 2
MOST = 64
N_ROW = 4
N_COL = 8


def block_flags(key, row_blocks, col_blocks, block_rows, block_cols, ceiling):
    number = row_blocks * col_blocks
    per_block = block_rows * block_cols
    first, second, third = jax.random.split(key, 3)
    counts = jax.random.randint(first, (number,), max(1, ceiling // 4), ceiling + 1)
    chosen = jax.random.randint(second, (), 0, number)
    counts = jnp.where(jnp.arange(number) == chosen, ceiling, counts)
    scores = jax.random.randint(third, (number, per_block), 0, 1 << 20) * per_block + jnp.arange(per_block)[None, :]
    order = jnp.argsort(scores, axis=1, stable=True)
    ranking = jnp.argsort(order, axis=1, stable=True)
    flags = (ranking < counts[:, None]).astype(jnp.int32)
    flags = flags.reshape(row_blocks, col_blocks, block_rows, block_cols).transpose(0, 2, 1, 3)
    return flags.reshape(row_blocks * block_rows, col_blocks * block_cols)


def draw_a_flags(key, part):
    return block_flags(jax.random.fold_in(key, 11), N_ROW, N_COL, TM_DEV, KT, MOST)


def draw_b_flags(key, part):
    return block_flags(jax.random.fold_in(key, 23), N_COL, N_COL, KT, TN_DEV, MOST)


def steps_of(own_key, shape, cuts, smallest, largest):
    factor_of, own = 1.0, jax.random.fold_in(own_key, 6)
    for dim, shards_of in cuts:
        heights = jnp.exp(jax.random.uniform(jax.random.fold_in(own, dim), (shards_of,), jnp.float32, smallest / len(cuts), largest / len(cuts)))
        factor_of = factor_of * jnp.repeat(heights, shape[dim] // shards_of).reshape([-1 if axis == dim else 1 for axis in range(len(shape))])
    return factor_of


def centred(own_key, shape, width, limit, cuts=(), held_as=jnp.bfloat16):
    drawn = width * jax.random.normal(own_key, shape, jnp.float32)
    if cuts:
        drawn = drawn * steps_of(own_key, shape, cuts, -0.22, 0.18)
    return jnp.clip(drawn, -limit, limit).astype(held_as)


def setup_inputs(seed: int = 0) -> dict:
    keys = jax.random.split(jax.random.key(seed), 6)
    a_matrix = centred(keys[0], (TILE * TM_DEV * N_ROW, TILE * KT * N_COL), 1.0, 6.0, ((0, 4), (1, 8)))
    a_flags = draw_a_flags(jax.random.fold_in(keys[5], 71), 0)
    b_matrix = centred(keys[2], (TILE * KT * N_COL, TILE * TN_DEV * N_COL), (KT * TILE) ** -0.5, 0.1875, ((0, 4), (1, 8)))
    b_flags = draw_b_flags(jax.random.fold_in(keys[5], 71), 0)
    sections = jax.random.randint(keys[4], (SECTIONS,), 0, N_COL).astype(jnp.int32)
    return {"a_matrix": a_matrix, "a_flags": a_flags, "b_matrix": b_matrix, "b_flags": b_flags, "sections": sections}


def mask_tiles(matrix, flags, tile_rows, tile_cols):
    shaped = matrix.reshape(tile_rows, TILE, tile_cols, TILE)
    shaped = shaped * flags.astype(matrix.dtype)[:, None, :, None]
    return shaped.reshape(tile_rows * TILE, tile_cols * TILE)


def to_tiles(matrix, tile_rows, tile_cols):
    return matrix.reshape(tile_rows, TILE, tile_cols, TILE).transpose(0, 2, 1, 3).reshape(tile_rows * tile_cols, TILE, TILE)


def from_tiles(tiles, tile_rows, tile_cols):
    return tiles.reshape(tile_rows, tile_cols, TILE, TILE).transpose(0, 2, 1, 3).reshape(tile_rows * TILE, tile_cols * TILE)


def compact(tiles, flags_flat, capacity):
    rank_of = jnp.cumsum(flags_flat) - 1
    slot_ids = jnp.arange(capacity, dtype=jnp.int32)
    matched = (flags_flat[None, :] == 1) & (rank_of[None, :] == slot_ids[:, None])
    source = jnp.sum(jnp.where(matched, jnp.arange(flags_flat.shape[0], dtype=jnp.int32)[None, :], 0), axis=1).astype(jnp.int32)
    is_valid = jnp.any(matched, axis=1)
    return jnp.take(tiles, source, axis=0) * is_valid.astype(tiles.dtype)[:, None, None]


def reference(a_matrix, a_flags, b_matrix, b_flags, sections):
    panel_width = KT * TILE

    def one_block(block):
        row_index = (block // N_COL).astype(jnp.int32)
        col_index = (block % N_COL).astype(jnp.int32)
        product = jnp.zeros((TM_DEV * TILE, TN_DEV * TILE), jnp.float32)
        intersection = jnp.zeros((TM_DEV, TN_DEV), jnp.float32)
        for step_index in range(SECTIONS):
            section = sections[step_index].astype(jnp.int32)
            a_panel = lax.dynamic_slice(a_matrix, (row_index * TM_DEV * TILE, section * panel_width), (TM_DEV * TILE, panel_width))
            a_panel_flags = lax.dynamic_slice(a_flags, (row_index * TM_DEV, section * KT), (TM_DEV, KT))
            b_panel = lax.dynamic_slice(b_matrix, (section * panel_width, col_index * TN_DEV * TILE), (panel_width, TN_DEV * TILE))
            b_panel_flags = lax.dynamic_slice(b_flags, (section * KT, col_index * TN_DEV), (KT, TN_DEV))
            a_masked = mask_tiles(a_panel, a_panel_flags, TM_DEV, KT)
            b_masked = mask_tiles(b_panel, b_panel_flags, KT, TN_DEV)
            product = product + jnp.dot(a_masked.astype(jnp.float32), b_masked.astype(jnp.float32), precision=lax.Precision.HIGHEST)
            intersection = intersection + jnp.dot(a_panel_flags.astype(jnp.float32), b_panel_flags.astype(jnp.float32), precision=lax.Precision.HIGHEST)
        occupied = (intersection > 0.5).astype(jnp.int32).reshape(-1)
        tiles = to_tiles(product.astype(jnp.bfloat16), TM_DEV, TN_DEV)
        packed_block = from_tiles(compact(tiles, occupied, TM_DEV * TN_DEV), TM_DEV, TN_DEV)
        return packed_block, jnp.sum(occupied).astype(jnp.int32)

    blocks, filled = lax.map(one_block, jnp.arange(N_ROW * N_COL, dtype=jnp.int32))
    offset = (jnp.cumsum(filled) - filled).astype(jnp.int32)
    slot_ids = jnp.arange(TM_DEV * TN_DEV, dtype=jnp.int32)
    places = jnp.where(slot_ids[None, :] < filled[:, None], offset[:, None] + slot_ids[None, :], -1).astype(jnp.int32)
    tile_place = places.reshape(N_ROW, N_COL, TM_DEV, TN_DEV).transpose(0, 2, 1, 3).reshape(N_ROW * TM_DEV, N_COL * TN_DEV)
    packed = blocks.reshape(N_ROW, N_COL, TM_DEV * TILE, TN_DEV * TILE).transpose(0, 2, 1, 3).reshape(N_ROW * TM_DEV * TILE, N_COL * TN_DEV * TILE)
    return packed, tile_place
```

```python
import functools

import jax
import jax.numpy as jnp
from jax import lax
from jax.experimental import pallas as pl
from jax.experimental.pallas import tpu as pltpu
from jax.sharding import PartitionSpec as P

TILE = 128
SECTIONS = 2
MOST = 64
CHUNKS = 16
MESH = pl.DeviceIdType.MESH
ANY = pl.BlockSpec(memory_space=pl.ANY)
SMEM = pl.BlockSpec(memory_space=pltpu.SMEM)
VMEM = pl.BlockSpec(memory_space=pltpu.VMEM)


def ring_place(index, n):
    half = n // 2
    turned = half + lax.rem(index - half + n // 4 + half, half)
    return jnp.where(index < half, index, turned)


def tile_at(ref, p, q):
    rows = pl.ds(pl.multiple_of(p * TILE, TILE), TILE)
    cols = pl.ds(pl.multiple_of(q * TILE, TILE), TILE)
    return ref.at[rows, cols]


def pack_kernel(tile_rows, panel, tile_cols, ratio, sections, a_flags, b_flags, a, b, a_out, b0_out, b1_out, sem):
    def gather(flags, src, out, rows, cols, first):
        def lap(i, rank):
            p, q = i // cols, lax.rem(i, cols)
            here = flags[first + p, q]

            @pl.when(here == 1)
            def _():
                pltpu.make_async_copy(tile_at(src, first + p, q), out.at[rank], sem).start()

            return rank + here

        return lax.fori_loop(0, rows * cols, lap, jnp.int32(0))

    total = jnp.int32(0)
    my_row, my_col = lax.axis_index("row"), lax.axis_index("col")
    mine_a = (sections[0] == my_col) | (sections[1] == my_col)
    total += lax.cond(mine_a, lambda: gather(a_flags, a, a_out, tile_rows, panel, 0), lambda: jnp.int32(0))
    for s, out in ((0, b0_out), (1, b1_out)):
        first = lax.rem(sections[s], ratio) * panel
        total += lax.cond(
            sections[s] // ratio == my_row,
            lambda: gather(b_flags, b, out, panel, tile_cols, first),
            lambda: jnp.int32(0),
        )

    @pl.loop(0, total)
    def _(i):
        pltpu.make_async_copy(tile_at(a, 0, 0), a_out.at[0], sem).wait()


def spread_kernel(root, owner, n_row, n_col, a_src, b_src, a_dst, b_dst, a_next, a_prev, a_recv, b_up, b_down, b_recv):
    my_row, my_col = lax.axis_index("row"), lax.axis_index("col")
    span = MOST // CHUNKS
    half = n_col // 2
    root_place = root if root < half else half + (root - half + n_col // 4) % half
    place = ring_place(my_col, n_col)
    dist = lax.rem(place - root_place + n_col, n_col)
    nxt = ring_place(lax.rem(place + 1, n_col), n_col)
    prv = ring_place(lax.rem(place + n_col - 1, n_col), n_col)
    a_root, b_root = dist == 0, my_row == owner
    to_next = dist < half
    to_prev = (dist == 0) | (dist > half + 1)
    to_up = (my_row >= owner) & (my_row < n_row - 1)
    to_down = (my_row <= owner) & (my_row > 0)
    up = jnp.minimum(my_row + 1, n_row - 1)
    down = jnp.maximum(my_row - 1, 0)

    barrier = pltpu.get_barrier_semaphore()

    def ready(when, row, col):
        @pl.when(when)
        def _():
            pl.semaphore_signal(barrier, inc=1, device_id=(row, col), device_id_type=MESH)

    ready((dist > 0) & (dist <= half), my_row, prv)
    ready(dist > half, my_row, nxt)
    ready(my_row > owner, down, my_col)
    ready(my_row < owner, up, my_col)
    targets = sum(when.astype(jnp.int32) for when in (to_next, to_prev, to_up, to_down))

    @pl.when(targets > 0)
    def _():
        pl.semaphore_wait(barrier, targets)

    def copy(src, dst, c, send, recv, row, col):
        part = pl.ds(c * span, span)
        return pltpu.make_async_remote_copy(
            src_ref=src.at[part],
            dst_ref=dst.at[part],
            send_sem=send.at[c],
            recv_sem=recv.at[c],
            device_id=(row, col),
            device_id_type=MESH,
        )

    def a_copies(src, c):
        return (
            (to_next, copy(src, a_dst, c, a_next, a_recv, my_row, nxt)),
            (to_prev, copy(src, a_dst, c, a_prev, a_recv, my_row, prv)),
        )

    def b_copies(src, c):
        return (
            (to_up, copy(src, b_dst, c, b_up, b_recv, up, my_col)),
            (to_down, copy(src, b_dst, c, b_down, b_recv, down, my_col)),
        )

    def start(copies):
        for when, one in copies:

            @pl.when(when)
            def _():
                one.start()

    @pl.when(b_root)
    def _():
        @pl.loop(0, CHUNKS)
        def _(c):
            start(b_copies(b_src, c))

    @pl.when(a_root)
    def _():
        @pl.loop(0, CHUNKS)
        def _(c):
            start(a_copies(a_src, c))

    def pass_a(c):
        @pl.when(jnp.logical_not(a_root))
        def _():
            copies = a_copies(a_dst, c)
            copies[0][1].wait_recv()
            start(copies)

    def pass_b(c):
        @pl.when(jnp.logical_not(b_root))
        def _():
            copies = b_copies(b_dst, c)
            copies[0][1].wait_recv()
            start(copies)

    lag = 2

    @pl.loop(0, CHUNKS)
    def _(c):
        pass_b(c)

        @pl.when((c >= lag) & (c < lag + CHUNKS // 2))
        def _():
            pass_a(2 * (c - lag))
            pass_a(2 * (c - lag) + 1)

    @pl.loop(0, CHUNKS)
    def _(c):
        for when, one in a_copies(a_dst, c) + b_copies(b_dst, c):

            @pl.when(when)
            def _():
                one.wait_send()


def spread(root, owner, n_row, n_col, a_src, b_src):
    return pl.pallas_call(
        functools.partial(spread_kernel, root, owner, n_row, n_col),
        out_shape=(
            jax.ShapeDtypeStruct(a_src.shape, a_src.dtype),
            jax.ShapeDtypeStruct(b_src.shape, b_src.dtype),
        ),
        in_specs=[ANY, ANY],
        out_specs=(ANY, ANY),
        scratch_shapes=[pltpu.SemaphoreType.DMA((CHUNKS,))] * 6,
        compiler_params=pltpu.CompilerParams(collective_id=root, has_side_effects=True),
        name=f"spread_{root}",
    )(a_src, b_src)


def product_kernel(
    tile_rows, panel, tile_cols, ratio, block, sections, a_flags, b_flags, slots, filled,
    a_mine, b0_mine, b1_mine, a0, a1, b0, b1, out, a_full, b_full, done, zero, sem, out_sem,
):
    my_row, my_col = lax.axis_index("row"), lax.axis_index("col")
    zero[...] = jnp.zeros_like(zero)
    slot_count = tile_rows * tile_cols

    def fill(flags, s, mine, got, is_mine, full, rows, cols, first_p, first_q):
        def lap(i, rank):
            p, q = i // cols, lax.rem(i, cols)
            here = flags[s, i]
            spot = tile_at(full, first_p + p, first_q + q)

            @pl.when((here == 1) & is_mine)
            def _():
                pltpu.make_async_copy(mine.at[rank], spot, sem).start()

            @pl.when((here == 1) & jnp.logical_not(is_mine))
            def _():
                pltpu.make_async_copy(got.at[rank], spot, sem).start()

            @pl.when(here == 0)
            def _():
                spot[...] = zero[...]

            return rank + here

        return lax.fori_loop(0, rows * cols, lap, jnp.int32(0))

    total = jnp.int32(0)
    for s, got_a, mine_b, got_b in ((0, a0, b0_mine, b0), (1, a1, b1_mine, b1)):
        total += fill(a_flags, s, a_mine, got_a, sections[s] == my_col, a_full, tile_rows, panel, 0, s * panel)
        total += fill(
            b_flags, s, mine_b, got_b, sections[s] // ratio == my_row, b_full, panel, tile_cols, s * panel, 0
        )

    @pl.loop(filled[0], slot_count)
    def _(k):
        pltpu.make_async_copy(zero, tile_at(out, k // tile_cols, lax.rem(k, tile_cols)), out_sem).start()

    @pl.loop(0, total)
    def _(i):
        pltpu.make_async_copy(a_mine.at[0], tile_at(a_full, 0, 0), sem).wait()

    across = tile_cols // block
    down = tile_rows // block

    @pl.loop(0, down * across)
    def _(step):
        i, j = step // across, lax.rem(step, across)
        rows = pl.ds(pl.multiple_of(i * block * TILE, block * TILE), block * TILE)
        cols = pl.ds(pl.multiple_of(j * block * TILE, block * TILE), block * TILE)
        done[rows, cols] = jnp.dot(
            a_full[rows, :], b_full[:, cols], preferred_element_type=jnp.float32
        ).astype(done.dtype)

    @pl.loop(0, slot_count)
    def _(i):
        slot = slots[i]

        @pl.when(slot >= 0)
        def _():
            pltpu.make_async_copy(
                tile_at(done, i // tile_cols, lax.rem(i, tile_cols)),
                tile_at(out, slot // tile_cols, lax.rem(slot, tile_cols)),
                out_sem,
            ).start()

    pltpu.make_async_copy(done, out, out_sem).wait()


def shards(n_row, n_col, a_matrix, a_flags, b_matrix, b_flags, sections):
    tile_rows, panel = a_flags.shape
    tile_cols = b_flags.shape[1]
    ratio = n_col // n_row
    dtype = a_matrix.dtype
    my_row, my_col = lax.axis_index("row"), lax.axis_index("col")

    tiles = jax.ShapeDtypeStruct((MOST, TILE, TILE), dtype)
    a_mine, b0_mine, b1_mine = pl.pallas_call(
        functools.partial(pack_kernel, tile_rows, panel, tile_cols, ratio),
        out_shape=(tiles, tiles, tiles),
        in_specs=[SMEM, SMEM, SMEM, ANY, ANY],
        out_specs=(VMEM, VMEM, VMEM),
        scratch_shapes=[pltpu.SemaphoreType.DMA],
        name="pack",
    )(sections, a_flags, b_flags, a_matrix, b_matrix)

    every = lax.all_gather(jnp.concatenate([a_flags, b_flags], axis=1), ("row", "col"))
    every = every.reshape(n_row, n_col, b_flags.shape[0], panel + tile_cols)

    got = []
    own_a, own_b = [], []
    common = jnp.zeros((n_row, n_col, tile_rows, tile_cols), jnp.float32)
    for s, b_mine in ((0, b0_mine), (1, b1_mine)):
        section = sections[s]
        branches = [
            functools.partial(spread, t, t // ratio, n_row, n_col) for t in range(n_col)
        ]
        got.append(lax.switch(section, branches, a_mine, b_mine))
        a_part = lax.dynamic_index_in_dim(every, section, 1, keepdims=False)[:, :, :panel]
        b_part = lax.dynamic_index_in_dim(every, section // ratio, 0, keepdims=False)
        b_part = lax.dynamic_slice_in_dim(b_part, section % ratio * panel, panel, 1)[:, :, panel:]
        own_a.append(lax.dynamic_index_in_dim(a_part, my_row, 0, keepdims=False).reshape(-1))
        own_b.append(lax.dynamic_index_in_dim(b_part, my_col, 0, keepdims=False).reshape(-1))
        common = common + jnp.einsum(
            "rpk,ckq->rcpq", a_part.astype(jnp.bfloat16), b_part.astype(jnp.bfloat16),
            preferred_element_type=jnp.float32,
        )
    occupied = (common > 0.5).astype(jnp.int32)
    counts = jnp.sum(occupied, axis=(2, 3)).reshape(-1)
    me = my_row * n_col + my_col
    offset = jnp.sum(jnp.where(jnp.arange(n_row * n_col) < me, counts, 0))
    own = occupied[my_row, my_col].reshape(-1)
    filled = jnp.sum(own)
    slots = jnp.where(own == 1, jnp.cumsum(own) - 1, -1).astype(jnp.int32)

    packed = pl.pallas_call(
        functools.partial(product_kernel, tile_rows, panel, tile_cols, ratio, 4),
        out_shape=jax.ShapeDtypeStruct((tile_rows * TILE, tile_cols * TILE), dtype),
        in_specs=[SMEM] * 5 + [ANY] * 7,
        out_specs=ANY,
        scratch_shapes=[
            pltpu.VMEM((tile_rows * TILE, SECTIONS * panel * TILE), dtype),
            pltpu.VMEM((SECTIONS * panel * TILE, tile_cols * TILE), dtype),
            pltpu.VMEM((tile_rows * TILE, tile_cols * TILE), dtype),
            pltpu.VMEM((TILE, TILE), dtype),
            pltpu.SemaphoreType.DMA,
            pltpu.SemaphoreType.DMA,
        ],
        compiler_params=pltpu.CompilerParams(vmem_limit_bytes=48 * 1024 * 1024),
        name="product",
    )(
        sections, jnp.stack(own_a), jnp.stack(own_b), slots, filled.reshape(1),
        a_mine, b0_mine, b1_mine, got[0][0], got[1][0], got[0][1], got[1][1],
    )
    slot_ids = jnp.arange(tile_rows * tile_cols, dtype=jnp.int32)
    places = jnp.where(slot_ids < filled, offset + slot_ids, -1).astype(jnp.int32)
    return packed, places.reshape(tile_rows, tile_cols)


def solution(mesh):
    return jax.shard_map(
        functools.partial(shards, mesh.shape["row"], mesh.shape["col"]),
        mesh=mesh,
        in_specs=(P("row", "col"), P("row", "col"), P("row", "col"), P("row", "col"), P()),
        out_specs=(P("row", "col"), P("row", "col")),
        check_vma=False,
    )
```

```python
import functools

import jax
import jax.numpy as jnp
from jax import lax
from jax.experimental import pallas as pl
from jax.experimental.pallas import tpu as pltpu
from jax.sharding import PartitionSpec as P

TILE = 128
SECTIONS = 2
MOST = 64
CHUNKS = 16
MESH = pl.DeviceIdType.MESH
ANY = pl.BlockSpec(memory_space=pl.ANY)
SMEM = pl.BlockSpec(memory_space=pltpu.SMEM)
VMEM = pl.BlockSpec(memory_space=pltpu.VMEM)


def ring_place(index, n):
    half = n // 2
    turned = half + lax.rem(index - half + n // 4 + half, half)
    return jnp.where(index < half, index, turned)


def tile_at(ref, p, q):
    rows = pl.ds(pl.multiple_of(p * TILE, TILE), TILE)
    cols = pl.ds(q * TILE if isinstance(q, int) else pl.multiple_of(q * TILE, TILE), TILE)
    return ref.at[rows, cols]


def pack_kernel(tile_rows, panel, tile_cols, ratio, sections, a_flags, b_flags, a, b, a_out, b0_out, b1_out, sem):
    def gather(flags, src, out, rows, cols, first):
        def lap(p, rank):
            for q in range(cols):
                here = flags[first + p, q]

                @pl.when(here == 1)
                def _():
                    pltpu.make_async_copy(tile_at(src, first + p, q), out.at[rank], sem).start()

                rank = rank + here
            return rank

        return lax.fori_loop(0, rows, lap, jnp.int32(0))

    total = jnp.int32(0)
    my_row, my_col = lax.axis_index("row"), lax.axis_index("col")
    mine_a = (sections[0] == my_col) | (sections[1] == my_col)
    total += lax.cond(mine_a, lambda: gather(a_flags, a, a_out, tile_rows, panel, 0), lambda: jnp.int32(0))
    for s, out in ((0, b0_out), (1, b1_out)):
        first = lax.rem(sections[s], ratio) * panel
        total += lax.cond(
            sections[s] // ratio == my_row,
            lambda: gather(b_flags, b, out, panel, tile_cols, first),
            lambda: jnp.int32(0),
        )

    @pl.loop(0, total)
    def _(i):
        pltpu.make_async_copy(tile_at(a, 0, 0), a_out.at[0], sem).wait()


def spread_kernel(root, owner, n_row, n_col, with_flags, *refs):
    if with_flags:
        a_src, b_src, flags, a_dst, b_dst, every, *sems = refs
        a_next, a_prev, a_recv, b_up, b_down, b_recv, local, row_send, row_recv, col_send, col_recv = sems
    else:
        a_src, b_src, a_dst, b_dst, a_next, a_prev, a_recv, b_up, b_down, b_recv = refs
    my_row, my_col = lax.axis_index("row"), lax.axis_index("col")
    span = MOST // CHUNKS
    half = n_col // 2
    root_place = root if root < half else half + (root - half + n_col // 4) % half
    place = ring_place(my_col, n_col)
    dist = lax.rem(place - root_place + n_col, n_col)
    nxt = ring_place(lax.rem(place + 1, n_col), n_col)
    prv = ring_place(lax.rem(place + n_col - 1, n_col), n_col)
    a_root, b_root = dist == 0, my_row == owner
    to_next = dist < half
    to_prev = (dist == 0) | (dist > half + 1)
    to_up = (my_row >= owner) & (my_row < n_row - 1)
    to_down = (my_row <= owner) & (my_row > 0)
    up = jnp.minimum(my_row + 1, n_row - 1)
    down = jnp.maximum(my_row - 1, 0)

    barrier = pltpu.get_barrier_semaphore()

    def ready(when, row, col):
        @pl.when(when)
        def _():
            pl.semaphore_signal(barrier, inc=1, device_id=(row, col), device_id_type=MESH)

    if with_flags:
        for k in range(1, n_row):
            ready(True, lax.rem(my_row + k, n_row), my_col)
        for k in range(1, n_col):
            ready(True, my_row, lax.rem(my_col + k, n_col))
        pl.semaphore_wait(barrier, n_row + n_col - 2)
    else:
        ready((dist > 0) & (dist <= half), my_row, prv)
        ready(dist > half, my_row, nxt)
        ready(my_row > owner, down, my_col)
        ready(my_row < owner, up, my_col)
        targets = sum(when.astype(jnp.int32) for when in (to_next, to_prev, to_up, to_down))

        @pl.when(targets > 0)
        def _():
            pl.semaphore_wait(barrier, targets)

    def along_row(k):
        return pltpu.make_async_remote_copy(
            src_ref=flags,
            dst_ref=every.at[my_col, my_row],
            send_sem=row_send.at[k],
            recv_sem=row_recv.at[k],
            device_id=(lax.rem(my_row + k, n_row), my_col),
            device_id_type=MESH,
        )

    def along_col(k):
        return pltpu.make_async_remote_copy(
            src_ref=every.at[my_col],
            dst_ref=every.at[my_col],
            send_sem=col_send.at[k],
            recv_sem=col_recv.at[k],
            device_id=(my_row, lax.rem(my_col + k, n_col)),
            device_id_type=MESH,
        )

    if with_flags:
        own = pltpu.make_async_copy(flags, every.at[my_col, my_row], local)
        own.start()
        for k in range(1, n_row):
            along_row(k).start()

    def copy(src, dst, c, send, recv, row, col):
        part = pl.ds(c * span, span)
        return pltpu.make_async_remote_copy(
            src_ref=src.at[part],
            dst_ref=dst.at[part],
            send_sem=send.at[c],
            recv_sem=recv.at[c],
            device_id=(row, col),
            device_id_type=MESH,
        )

    def a_copies(src, c):
        return (
            (to_next, copy(src, a_dst, c, a_next, a_recv, my_row, nxt)),
            (to_prev, copy(src, a_dst, c, a_prev, a_recv, my_row, prv)),
        )

    def b_copies(src, c):
        return (
            (to_up, copy(src, b_dst, c, b_up, b_recv, up, my_col)),
            (to_down, copy(src, b_dst, c, b_down, b_recv, down, my_col)),
        )

    def start(copies):
        for when, one in copies:

            @pl.when(when)
            def _():
                one.start()

    @pl.when(b_root)
    def _():
        @pl.loop(0, CHUNKS)
        def _(c):
            start(b_copies(b_src, c))

    @pl.when(a_root)
    def _():
        @pl.loop(0, CHUNKS)
        def _(c):
            start(a_copies(a_src, c))

    def pass_a(c):
        @pl.when(jnp.logical_not(a_root))
        def _():
            copies = a_copies(a_dst, c)
            copies[0][1].wait_recv()
            start(copies)

    def pass_b(c):
        @pl.when(jnp.logical_not(b_root))
        def _():
            copies = b_copies(b_dst, c)
            copies[0][1].wait_recv()
            start(copies)

    if with_flags:
        own.wait()
        for k in range(1, n_row):
            along_row(k).wait_recv()
        for k in range(1, n_col):
            along_col(k).start()

    lag = 2

    @pl.loop(0, CHUNKS)
    def _(c):
        pass_b(c)

        @pl.when((c >= lag) & (c < lag + CHUNKS // 2))
        def _():
            pass_a(2 * (c - lag))
            pass_a(2 * (c - lag) + 1)

    @pl.loop(0, CHUNKS)
    def _(c):
        for when, one in a_copies(a_dst, c) + b_copies(b_dst, c):

            @pl.when(when)
            def _():
                one.wait_send()

    if with_flags:
        for k in range(1, n_row):
            along_row(k).wait_send()
        for k in range(1, n_col):
            along_col(k).wait()


def spread(root, owner, n_row, n_col, a_src, b_src, flags=None):
    shapes = [jax.ShapeDtypeStruct(x.shape, x.dtype) for x in (a_src, b_src)]
    operands = [a_src, b_src]
    sems = [pltpu.SemaphoreType.DMA((CHUNKS,))] * 6
    if flags is not None:
        operands.append(flags)
        shapes.append(jax.ShapeDtypeStruct((n_col, n_row) + flags.shape, flags.dtype))
        sems += [pltpu.SemaphoreType.DMA] + [pltpu.SemaphoreType.DMA((n,)) for n in (n_row, n_row, n_col, n_col)]
    return pl.pallas_call(
        functools.partial(spread_kernel, root, owner, n_row, n_col, flags is not None),
        out_shape=tuple(shapes),
        in_specs=[ANY] * len(operands),
        out_specs=(ANY,) * len(shapes),
        scratch_shapes=sems,
        compiler_params=pltpu.CompilerParams(
            collective_id=root + (n_col if flags is None else 0), has_side_effects=True
        ),
        name=f"spread_{root}" if flags is None else f"spread_flags_{root}",
    )(*operands)


def product_kernel(
    tile_rows, panel, tile_cols, ratio, block, sections, a_flags, b_flags, slots, filled,
    a_mine, b0_mine, b1_mine, a0, a1, b0, b1, out, a_full, b_full, done, zero, sem, out_sem,
):
    my_row, my_col = lax.axis_index("row"), lax.axis_index("col")
    zero[...] = jnp.zeros_like(zero)
    slot_count = tile_rows * tile_cols

    def fill(flags, s, mine, got, is_mine, full, rows, cols, first_p, first_q):
        def run(src):
            def lap(p, rank):
                for q in range(cols):
                    here = flags[s, p * cols + q]
                    spot = tile_at(full, first_p + p, first_q + q)

                    @pl.when(here == 1)
                    def _():
                        pltpu.make_async_copy(src.at[rank], spot, sem).start()

                    @pl.when(here == 0)
                    def _():
                        spot[...] = jnp.zeros((TILE, TILE), full.dtype)

                    rank = rank + here
                return rank

            return lax.fori_loop(0, rows, lap, jnp.int32(0))

        return lax.cond(is_mine, lambda: run(mine), lambda: run(got))

    total = jnp.int32(0)
    for s, got_a, mine_b, got_b in ((0, a0, b0_mine, b0), (1, a1, b1_mine, b1)):
        total += fill(a_flags, s, a_mine, got_a, sections[s] == my_col, a_full, tile_rows, panel, 0, s * panel)
        total += fill(
            b_flags, s, mine_b, got_b, sections[s] // ratio == my_row, b_full, panel, tile_cols, s * panel, 0
        )

    @pl.loop(filled[0], slot_count)
    def _(k):
        pltpu.make_async_copy(zero, tile_at(out, k // tile_cols, lax.rem(k, tile_cols)), out_sem).start()

    @pl.loop(0, total)
    def _(i):
        pltpu.make_async_copy(a_mine.at[0], tile_at(a_full, 0, 0), sem).wait()

    across = tile_cols // block
    down = tile_rows // block

    @pl.loop(0, down)
    def _(i):
        rows = pl.ds(pl.multiple_of(i * block * TILE, block * TILE), block * TILE)

        @pl.loop(0, across)
        def _(j):
            cols = pl.ds(pl.multiple_of(j * block * TILE, block * TILE), block * TILE)
            done[rows, cols] = jnp.dot(
                a_full[rows, :], b_full[:, cols], preferred_element_type=jnp.float32
            ).astype(done.dtype)

        @pl.loop(0, block)
        def _(r):
            p = i * block + r
            for q in range(tile_cols):
                slot = slots[p * tile_cols + q]

                @pl.when(slot >= 0)
                def _():
                    pltpu.make_async_copy(
                        tile_at(done, p, q),
                        tile_at(out, lax.div(slot, tile_cols), lax.rem(slot, tile_cols)),
                        out_sem,
                    ).start()

    pltpu.make_async_copy(done, out, out_sem).wait()


def shards(n_row, n_col, a_matrix, a_flags, b_matrix, b_flags, sections):
    tile_rows, panel = a_flags.shape
    tile_cols = b_flags.shape[1]
    ratio = n_col // n_row
    dtype = a_matrix.dtype
    my_row, my_col = lax.axis_index("row"), lax.axis_index("col")

    tiles = jax.ShapeDtypeStruct((MOST, TILE, TILE), dtype)
    a_mine, b0_mine, b1_mine = pl.pallas_call(
        functools.partial(pack_kernel, tile_rows, panel, tile_cols, ratio),
        out_shape=(tiles, tiles, tiles),
        in_specs=[SMEM, SMEM, SMEM, ANY, ANY],
        out_specs=(VMEM, VMEM, VMEM),
        scratch_shapes=[pltpu.SemaphoreType.DMA],
        name="pack",
    )(sections, a_flags, b_flags, a_matrix, b_matrix)

    flags = jnp.concatenate([a_flags, b_flags], axis=1)
    flags = jnp.pad(flags, ((0, 0), (0, -flags.shape[1] % TILE)))
    got = []
    for s, b_mine in ((0, b0_mine), (1, b1_mine)):
        operands = (a_mine, b_mine) if s else (a_mine, b_mine, flags)
        branches = [functools.partial(spread, t, t // ratio, n_row, n_col) for t in range(n_col)]
        got.append(lax.switch(sections[s], branches, *operands))
    every = got[0][2]

    own_a, own_b = [], []
    common = jnp.zeros((n_row, n_col, tile_rows, tile_cols), jnp.float32)
    for s in range(SECTIONS):
        section = sections[s]
        a_part = lax.dynamic_index_in_dim(every, section, 0, keepdims=False)[:, :, :panel]
        b_part = lax.dynamic_index_in_dim(every, section // ratio, 1, keepdims=False)
        b_part = lax.dynamic_slice_in_dim(b_part, section % ratio * panel, panel, 1)[:, :, panel : panel + tile_cols]
        own_a.append(lax.dynamic_index_in_dim(a_part, my_row, 0, keepdims=False).reshape(-1))
        own_b.append(lax.dynamic_index_in_dim(b_part, my_col, 0, keepdims=False).reshape(-1))
        common = common + jnp.einsum(
            "rpk,ckq->rcpq", a_part.astype(jnp.bfloat16), b_part.astype(jnp.bfloat16),
            preferred_element_type=jnp.float32,
        )
    occupied = (common > 0.5).astype(jnp.int32)
    counts = jnp.sum(occupied, axis=(2, 3)).reshape(-1)
    me = my_row * n_col + my_col
    offset = jnp.sum(jnp.where(jnp.arange(n_row * n_col) < me, counts, 0))
    own = occupied[my_row, my_col].reshape(-1)
    filled = jnp.sum(own)
    slots = jnp.where(own == 1, jnp.cumsum(own) - 1, -1).astype(jnp.int32)

    packed = pl.pallas_call(
        functools.partial(product_kernel, tile_rows, panel, tile_cols, ratio, 4),
        out_shape=jax.ShapeDtypeStruct((tile_rows * TILE, tile_cols * TILE), dtype),
        in_specs=[SMEM] * 5 + [ANY] * 7,
        out_specs=ANY,
        scratch_shapes=[
            pltpu.VMEM((tile_rows * TILE, SECTIONS * panel * TILE), dtype),
            pltpu.VMEM((SECTIONS * panel * TILE, tile_cols * TILE), dtype),
            pltpu.VMEM((tile_rows * TILE, tile_cols * TILE), dtype),
            pltpu.VMEM((TILE, TILE), dtype),
            pltpu.SemaphoreType.DMA,
            pltpu.SemaphoreType.DMA,
        ],
        compiler_params=pltpu.CompilerParams(vmem_limit_bytes=48 * 1024 * 1024),
        name="product",
    )(
        sections, jnp.stack(own_a), jnp.stack(own_b), slots, filled.reshape(1),
        a_mine, b0_mine, b1_mine, got[0][0], got[1][0], got[0][1], got[1][1],
    )
    slot_ids = jnp.arange(tile_rows * tile_cols, dtype=jnp.int32)
    places = jnp.where(slot_ids < filled, offset + slot_ids, -1).astype(jnp.int32)
    return packed, places.reshape(tile_rows, tile_cols)


def solution(mesh):
    return jax.shard_map(
        functools.partial(shards, mesh.shape["row"], mesh.shape["col"]),
        mesh=mesh,
        in_specs=(P("row", "col"), P("row", "col"), P("row", "col"), P("row", "col"), P()),
        out_specs=(P("row", "col"), P("row", "col")),
        check_vma=False,
    )
```
